32 devices in a mesh: group: 2 (over y), tm: 4 (over z), space: 2 (over x), head: 2 (over core).
Axes of the slice: x: 2, y: 2, z: 4, core: 2. Of those that a mesh axis runs over, the one named last changes fastest.
Arguments:
- queries: bfloat16 [8, 16, 32, 3072], P(('group', 'tm'), 'space', None, 'head'), parts along dimension 0, may hold values from -5.5 to 5.5
- keys: bfloat16 [8, 16, 32, 3072], P(('group', 'tm'), 'space', None, 'head'), parts along dimension 0, may hold values from -5.5 to 5.5
- values: bfloat16 [8, 16, 32, 3072], P(('group', 'tm'), 'space', None, 'head'), parts along dimension 0, may hold values from -6 to 6
- window: int32 [8, 2, 4, 27], P(('group', 'tm'), 'space'), parts along dimension 0, may hold values 0 or 1
Outputs:
- attended: bfloat16 [8, 16, 32, 3072], P(('group', 'tm'), 'space', None, 'head'), parts along dimension 0
The draws below stay inside these ranges and needn't reach their ends.
There are 2 independent parts, one for each index of `group`. The reference program is written for one: setup_inputs(seed, part) draws one part's arguments, and reference() takes and returns one part's arrays. A program takes and returns all parts, laid end to end along the dimension named above; each array names one. Nothing has to cross between parts.
Inputs may be any that keep to these rules, and one draw needn't show every extreme that they name: `window`: slot dt * 9 + (dy + 1) * 3 + (dx + 1) of a query tile's entry enables the key tile dt frames earlier, dy tile rows and dx tile columns away; slot 4, the tile itself, is attended whatever it holds.
All inputs are finite; a program needn't handle non-finite values. No bound on the sum of `window` on one device may be relied on, other than what follows from the above.
Results may differ from the reference program's by a relative error of at most 0.0046.
Values may be sent and summed in bfloat16 or wider, within the bound.
A program may use at most 128 MiB of HBM per device.

```python
import jax
import jax.numpy as jnp
from jax import lax

HEADS = 24
HDIM = 128
TILE = 8
TCOLS = 4
FRAMES = 4
TROWS = 2
ROWS = 16
COLS = 32


def base_field(key, salt):
    shape = (FRAMES, ROWS, COLS, HEADS * HDIM)
    local_key = jax.random.fold_in(key, salt)
    return jnp.clip(jax.random.normal(local_key, shape, jnp.float32), -4.0, 4.0)


def draw_queries(key, part):
    base = base_field(key, 1)
    return base.astype(jnp.bfloat16)


def draw_keys(key, part):
    base = base_field(key, 2)
    return base.astype(jnp.bfloat16)


def plant(entries, rng, smallest, high):
    shape = entries.shape
    index_at = [jax.random.randint(jax.random.fold_in(rng, axis), (), 0, shape[axis]) for axis in range(len(shape))]
    entries = entries.at[tuple(index_at)].set(smallest)
    longest = shape.index(max(shape))
    index_at[longest] = (index_at[longest] + 1) % shape[longest]
    return entries.at[tuple(index_at)].set(high)


def shard_levels(stream_key, dims, split, low, top_value):
    loudness, own = 1.0, jax.random.fold_in(stream_key, 6)
    for dim, shards_of in split:
        draws = jnp.exp(jax.random.uniform(jax.random.fold_in(own, dim), (shards_of,), jnp.float32, low / len(split), top_value / len(split)))
        loudness = loudness * jnp.repeat(draws, dims[dim] // shards_of).reshape([-1 if axis == dim else 1 for axis in range(len(dims))])
    return loudness


def bell_draw(key, extent, deviation, limit, shards=(), held_as=jnp.bfloat16):
    level = shard_levels(key, extent, shards, -0.22, 0.18) if shards else 1.0
    entries = jax.random.normal(key, extent, jnp.float32) * deviation * level
    return jnp.minimum(jnp.maximum(entries, -limit), limit).astype(held_as)


def setup_inputs(seed: int = 0, part: int = 0) -> dict:
    key_list = jax.random.split(jax.random.key(seed), 5)
    own_keys = jax.random.split(jax.random.fold_in(key_list[4], part), 5)
    return {
        "queries": draw_queries(jax.random.fold_in(jax.random.fold_in(key_list[4], part), 71), part),
        "keys": draw_keys(jax.random.fold_in(jax.random.fold_in(key_list[4], part), 71), part),
        "values": bell_draw(own_keys[2], (FRAMES, ROWS, COLS, HEADS * HDIM), 1.0, 6.0, ((0, 4), (1, 2), (3, 2))),
        "window": plant((jax.random.randint(own_keys[3], (FRAMES, TROWS, TCOLS, 27), 0, 3) < 2).astype(jnp.int32), jax.random.fold_in(own_keys[3], 1), 0, 1),
    }


def reference(queries, keys, values, window):
    channels = HEADS * HDIM
    pad_spec = ((2, 0), (TILE, TILE), (TILE, TILE), (0, 0))
    keys_padded = jnp.pad(keys, pad_spec)
    values_padded = jnp.pad(values, pad_spec)
    score_scale = HDIM ** -0.5
    steps_back = jnp.arange(3, dtype=jnp.int32)
    shifts = jnp.arange(3, dtype=jnp.int32) - 1
    slot_of = steps_back[:, None, None] * 9 + (shifts[None, :, None] + 1) * 3 + shifts[None, None, :] + 1
    slot_ids = jnp.arange(27, dtype=jnp.int32)
    zero_idx = jnp.int32(0)

    def attend(tile_id):
        frame = tile_id // (TROWS * TCOLS)
        tile_row = (tile_id // TCOLS) % TROWS
        tile_col = tile_id % TCOLS
        query_tile = lax.dynamic_slice(queries, (frame, tile_row * TILE, tile_col * TILE, zero_idx), (1, TILE, TILE, channels))
        query_tile = query_tile.reshape(TILE * TILE, HEADS, HDIM).astype(jnp.float32)
        key_block = lax.dynamic_slice(keys_padded, (frame, tile_row * TILE, tile_col * TILE, zero_idx), (3, 3 * TILE, 3 * TILE, channels))[::-1]
        value_block = lax.dynamic_slice(values_padded, (frame, tile_row * TILE, tile_col * TILE, zero_idx), (3, 3 * TILE, 3 * TILE, channels))[::-1]
        key_rows = key_block.reshape(27 * TILE * TILE, HEADS, HDIM).astype(jnp.float32)
        value_rows = value_block.reshape(27 * TILE * TILE, HEADS, HDIM).astype(jnp.float32)
        frame_ok = frame - steps_back >= 0
        row_ok = (tile_row + shifts >= 0) & (tile_row + shifts < TROWS)
        col_ok = (tile_col + shifts >= 0) & (tile_col + shifts < TCOLS)
        bits_row = lax.dynamic_slice(window, (frame, tile_row, tile_col, zero_idx), (1, 1, 1, 27)).reshape(27)
        picked = jnp.sum(jnp.where(slot_of[..., None] == slot_ids, bits_row, 0), axis=-1)
        allowed = ((picked == 1) | (slot_of == 4)) & frame_ok[:, None, None] & row_ok[None, :, None] & col_ok[None, None, :]
        key_ok = jnp.broadcast_to(allowed[:, :, None, :, None], (3, 3, TILE, 3, TILE)).reshape(27 * TILE * TILE)
        scores = jnp.einsum("qhd,khd->hqk", query_tile, key_rows) * score_scale
        scores = jnp.where(key_ok, scores, -jnp.inf)
        row_max = jnp.max(scores, axis=-1, keepdims=True)
        weights = jnp.exp(scores - row_max)
        row_sum = jnp.sum(weights, axis=-1)
        weights_bf = lax.optimization_barrier(weights.astype(jnp.bfloat16)).astype(jnp.float32)
        numerator = jnp.einsum("hqk,khd->qhd", weights_bf, value_rows)
        result = numerator / row_sum.T[:, :, None]
        return result.astype(jnp.bfloat16).reshape(TILE, TILE, channels)

    per_tile = lax.map(attend, jnp.arange(FRAMES * TROWS * TCOLS, dtype=jnp.int32))
    per_tile = per_tile.reshape(FRAMES, TROWS, TCOLS, TILE, TILE, channels)
    return per_tile.transpose(0, 1, 3, 2, 4, 5).reshape(FRAMES, ROWS, COLS, channels)
```

```python
import functools
import math

import jax
import jax.numpy as jnp
from jax import lax
from jax.experimental import pallas as pl
from jax.experimental.pallas import tpu as pltpu
from jax.sharding import PartitionSpec as P

HDIM = 128
TILE = 8
LANES = 128
OWN_AHEAD = 3
FAR_LAG, PASS_LAG, LAST_LAG = 1, 2, 5
MASKED = -float(2**17)
EXP2_SCALE = HDIM ** (-0.5) * math.log2(math.e)
VMEM_LIMIT = 40 * 2**20
MESH = pl.DeviceIdType.MESH


def remote(src, dst, send_sem, recv_sem, device):
    return pltpu.make_async_remote_copy(
        src_ref=src,
        dst_ref=dst,
        send_sem=send_sem,
        recv_sem=recv_sem,
        device_id=device,
        device_id_type=MESH,
    )


def kernel(
    frames,
    rows,
    q_hbm,
    k_hbm,
    v_hbm,
    win_hbm,
    out_ref,
    q_all,
    kv_all,
    qb_all,
    kone,
    o_send,
    o_recv,
    o_own,
    lse_own,
    win_ref,
    load_sem,
    win_sem,
    kv_send_sem,
    kv_recv_sem,
    q_send_sem,
    q_recv_sem,
    o_send_sem,
    o_recv_sem,
):
    frame = lax.axis_index("tm")
    row = lax.axis_index("space")
    heads = q_all.shape[1]
    columns = q_all.shape[3]
    tile_cols = columns // TILE
    tokens = TILE * columns
    has1 = frame + 1 < frames
    has2 = frame + 2 < frames
    prev1 = frame >= 1
    if rows == 1:
        sides = []
    elif rows == 2:
        sides = [(0, 1 - row, None, 1 - 2 * row, 0)]
    else:
        sides = [(0, row - 1, row >= 1, -1, 1), (1, row + 1, row + 1 < rows, 1, 0)]

    def when(*conditions):
        conditions = [c for c in conditions if c is not None]
        if not conditions:
            return lambda body: body()
        return pl.when(functools.reduce(jnp.logical_and, conditions))

    def load(head):
        lanes = pl.ds(pl.multiple_of(head * HDIM, HDIM), HDIM)
        return [
            pltpu.make_async_copy(src.at[0, :, :, lanes], dst, load_sem.at[head, i])
            for i, (src, dst) in enumerate(
                (
                    (k_hbm, kv_all.at[0, head, 0]),
                    (v_hbm, kv_all.at[0, head, 1]),
                    (q_hbm, q_all.at[0, head]),
                )
            )
        ]

    def send_kv(side, head):
        slot, there, _, _, far_slot = side
        return remote(
            kv_all.at[0, head],
            kv_all.at[1 + far_slot, head],
            kv_send_sem.at[slot, head],
            kv_recv_sem.at[far_slot, head],
            {"space": there},
        )

    def got_kv(side, head):
        slot, there, _, _, _ = side
        return remote(
            kv_all.at[0, head],
            kv_all.at[1 + slot, head],
            kv_send_sem.at[slot, head],
            kv_recv_sem.at[slot, head],
            {"space": there},
        )

    def send_q(stage, head):
        return remote(
            q_all.at[stage, head],
            q_all.at[stage + 1, head],
            q_send_sem.at[stage, head],
            q_recv_sem.at[stage, head],
            {"tm": frame - 1},
        )

    def send_qb(stage):
        return remote(
            qb_all.at[stage],
            qb_all.at[stage + 1],
            q_send_sem.at[stage, heads],
            q_recv_sem.at[stage, heads],
            {"tm": frame - 1},
        )

    def send_o(dt, head):
        return remote(
            o_send.at[dt - 1, head],
            o_recv.at[dt - 1, head],
            o_send_sem.at[dt - 1, head],
            o_recv_sem.at[dt - 1, head],
            {"tm": frame + 1},
        )

    def each_head(body):
        def step(head, carry):
            body(head)
            return carry

        lax.fori_loop(0, heads, step, 0)

    partners = [({"space": side[1]}, side[2]) for side in sides] + [
        ({"tm": frame + 1}, has1),
        ({"tm": frame - 1}, prev1),
    ]
    barrier = pltpu.get_barrier_semaphore()
    for device, there in partners:

        @when(there)
        def _():
            pl.semaphore_signal(barrier, inc=1, device_id=device, device_id_type=MESH)

    window = pltpu.make_async_copy(win_hbm, win_ref, win_sem)
    for copy in load(0):
        copy.start()
    window.start()

    def load_rest(head, carry):
        for copy in load(head):
            copy.start()
        return carry

    lax.fori_loop(1, heads, load_rest, 0)

    peers = sum(
        1 if there is None else jnp.where(there, 1, 0).astype(jnp.int32) for _, there in partners
    )
    pl.semaphore_wait(barrier, peers)

    def launch(head, own):
        for copy in load(head):
            copy.wait()
        for side in sides:

            @when(side[2])
            def _():
                send_kv(side, head).start()

        if own:

            @when(prev1)
            def _():
                send_q(0, head).start()

    ahead = min(OWN_AHEAD, heads)
    for head in range(ahead):
        launch(head, True)

    window.wait()
    lane = lax.broadcasted_iota(jnp.int32, (1, HDIM), 1)
    lane_row = lane // tile_cols
    lane_col = lane % tile_cols
    lane_dy = lane_row % 3 - 1
    row_ok = (row + lane_dy >= 0) & (row + lane_dy < rows) & (lane_row < 9)
    col_of = lax.broadcasted_iota(jnp.int32, (columns, 1), 0) // TILE
    table = jnp.zeros((columns, HDIM), jnp.float32)
    for col in range(tile_cols):
        dx = lane_col - col
        near = row_ok & (dx >= -1) & (dx <= 1)
        slot_of = lane_row * 3 + dx + 1
        picked = jnp.zeros((1, HDIM), jnp.int32)
        for slot in range(27):
            picked = jnp.where(slot_of == slot, win_ref[0, 0, col, slot], picked)
        allowed = near & ((picked == 1) | (slot_of == 4))
        offsets = jnp.where(allowed, 0.0, MASKED)
        table = jnp.where(col_of == col, offsets, table)
    qb_all[0] = table.astype(jnp.bfloat16)

    @when(prev1)
    def _():
        send_qb(0).start()

    def launch_rest(head, carry):
        launch(head, False)
        return carry

    lax.fori_loop(ahead, heads, launch_rest, 0)

    token = lax.broadcasted_iota(jnp.int32, (tokens, HDIM), 0)
    key_col = (token % columns) // TILE
    key_lane = lax.broadcasted_iota(jnp.int32, (tokens, HDIM), 1)
    for dt in range(3):
        for block, dy in enumerate([0] + [side[3] for side in sides]):
            hot = (dt * 3 + dy + 1) * tile_cols + key_col == key_lane
            kone[dt, pl.ds(block * tokens, tokens), :] = jnp.where(hot, 1.0, 0.0).astype(
                jnp.bfloat16
            )

    for side in sides:
        if side[2] is not None:

            @when(jnp.logical_not(side[2]))
            def _():
                @each_head
                def _(head):
                    kv_all[1 + side[0], head] = jnp.zeros(kv_all.shape[2:], jnp.bfloat16)

    blocks = range(1 + len(sides))

    def attend(dt, head):
        query = q_all[dt, head].reshape(tokens, HDIM)
        offsets = jnp.concatenate([qb_all[dt]] * TILE, axis=0)
        query = jnp.concatenate([query, offsets], axis=1)
        key = jnp.concatenate([kv_all[b, head, 0].reshape(tokens, HDIM) for b in blocks], axis=0)
        key = jnp.concatenate([key, kone[dt]], axis=1)
        value = jnp.concatenate([kv_all[b, head, 1].reshape(tokens, HDIM) for b in blocks], axis=0)
        scores = lax.dot_general(
            key, query, (((1,), (1,)), ((), ())), preferred_element_type=jnp.float32
        )
        top = jnp.max(scores, axis=0, keepdims=True)
        weights = jnp.exp2((scores - top) * EXP2_SCALE)
        total = jnp.sum(weights, axis=0, keepdims=True)
        part = lax.dot_general(
            value,
            weights.astype(jnp.bfloat16),
            (((0,), (0,)), ((), ())),
            preferred_element_type=jnp.float32,
        )
        return part / total, top * EXP2_SCALE + jnp.log2(total)

    chunks = tokens // LANES
    extra_row = lax.broadcasted_iota(jnp.int32, (o_send.shape[2] - chunks * HDIM, LANES), 0)

    def pack(dt, head, part, lse):
        high = lse.astype(jnp.bfloat16).astype(jnp.float32)
        middle = (lse - high).astype(jnp.bfloat16).astype(jnp.float32)
        low = lse - high - middle
        extra = jnp.zeros(extra_row.shape, jnp.float32)
        for chunk in range(chunks):
            lanes = slice(chunk * LANES, (chunk + 1) * LANES)
            o_send[dt - 1, head, pl.ds(chunk * HDIM, HDIM), :] = part[:, lanes].astype(jnp.bfloat16)
            for word, values in enumerate((high, middle, low)):
                extra = jnp.where(extra_row == chunk * 3 + word, values[:, lanes], extra)
        o_send[dt - 1, head, pl.ds(chunks * HDIM, extra_row.shape[0]), :] = extra.astype(
            jnp.bfloat16
        )

    def unpack(dt, head):
        extra = o_recv[dt - 1, head, pl.ds(chunks * HDIM, extra_row.shape[0]), :].astype(jnp.float32)
        parts, lses = [], []
        for chunk in range(chunks):
            parts.append(o_recv[dt - 1, head, pl.ds(chunk * HDIM, HDIM), :].astype(jnp.float32))
            first = chunk * 3
            lses.append(extra[first : first + 1] + extra[first + 1 : first + 2] + extra[first + 2 : first + 3])
        return jnp.concatenate(parts, axis=1), jnp.concatenate(lses, axis=1)

    def keep(dt, head, part, lse):
        o_own[dt, head] = part
        lse_own[dt, head] = jnp.broadcast_to(lse, lse_own.shape[2:])

    def kept(dt, head):
        return o_own[dt, head], lse_own[dt, head][:1]

    def merge(one, two):
        top = jnp.maximum(one[1], two[1])
        share_one, share_two = jnp.exp2(one[1] - top), jnp.exp2(two[1] - top)
        total = share_one + share_two
        part = one[0] * (share_one / total) + two[0] * (share_two / total)
        return part, top + jnp.log2(total)

    def finish(head, part):
        lanes = pl.ds(pl.multiple_of(head * HDIM, HDIM), HDIM)
        out_ref[0, :, :, lanes] = part.T.astype(jnp.bfloat16).reshape(TILE, columns, HDIM)

    def relay(head):
        @when(has1, head < heads)
        def _():
            send_q(0, head).wait_recv()

            @when(prev1)
            def _():
                send_q(1, head).start()

    def inside(head):
        return (head >= 0) & (head < heads)

    relay(jnp.int32(0))

    @when(has1)
    def _():
        send_qb(0).wait_recv()

        @when(prev1)
        def _():
            send_qb(1).start()

    def step(i, carry):
        far, passing, last = i - FAR_LAG, i - PASS_LAG, i - LAST_LAG

        @when(inside(far), has2)
        def _():
            @when(far == 0)
            def _():
                send_qb(1).wait_recv()

            send_q(1, far).wait_recv()
            pack(2, far, *attend(2, far))
            send_o(2, far).start()

        relay(i + 1)

        @when(i < heads)
        def _():
            for side in sides:

                @when(side[2])
                def _():
                    got_kv(side, i).wait_recv()

            @when(has1)
            def _():
                keep(1, i, *attend(1, i))

        @when(inside(passing), has1)
        def _():
            @when(prev1)
            def _():
                send_o(2, passing).wait_recv()
                pack(1, passing, *merge(kept(1, passing), unpack(2, passing)))

            @when(jnp.logical_not(prev1))
            def _():
                pack(1, passing, *kept(1, passing))

            send_o(1, passing).start()

        @when(i < heads)
        def _():
            keep(0, i, *attend(0, i))

        @when(prev1, i + ahead < heads)
        def _():
            send_q(0, i + ahead).start()

        @when(inside(last))
        def _():
            @when(prev1)
            def _():
                send_o(1, last).wait_recv()
                finish(last, merge(kept(0, last), unpack(1, last))[0])

            @when(jnp.logical_not(prev1))
            def _():
                finish(last, o_own[0, last])

        return carry

    lax.fori_loop(0, heads + LAST_LAG, step, 0)

    @when(prev1)
    def _():
        send_qb(0).wait_send()

        @when(has1)
        def _():
            send_qb(1).wait_send()

    @each_head
    def _(head):
        for side in sides:

            @when(side[2])
            def _():
                send_kv(side, head).wait_send()

        @when(prev1)
        def _():
            send_q(0, head).wait_send()

            @when(has1)
            def _():
                send_q(1, head).wait_send()

        @when(has1)
        def _():
            send_o(1, head).wait_send()

        @when(has2)
        def _():
            send_o(2, head).wait_send()


def solution(mesh):
    frames, rows = mesh.shape["tm"], mesh.shape["space"]

    def on_device(queries, keys, values, window):
        _, _, columns, channels = queries.shape
        heads = channels // HDIM
        tokens = TILE * columns
        beside = min(rows - 1, 2)
        block = (TILE, columns, HDIM)
        chunks = tokens // LANES
        packed = chunks * HDIM + -(-3 * chunks // 8) * 8
        dma = pltpu.SemaphoreType.DMA
        return pl.pallas_call(
            functools.partial(kernel, frames, rows),
            out_shape=jax.ShapeDtypeStruct(queries.shape, jnp.bfloat16),
            in_specs=[pl.BlockSpec(memory_space=pl.ANY)] * 4,
            out_specs=pl.BlockSpec(memory_space=pltpu.VMEM),
            scratch_shapes=[
                pltpu.VMEM((3, heads, *block), jnp.bfloat16),
                pltpu.VMEM((1 + beside, heads, 2, *block), jnp.bfloat16),
                pltpu.VMEM((3, columns, HDIM), jnp.bfloat16),
                pltpu.VMEM((3, (1 + beside) * tokens, HDIM), jnp.bfloat16),
                pltpu.VMEM((2, heads, packed, LANES), jnp.bfloat16),
                pltpu.VMEM((2, heads, packed, LANES), jnp.bfloat16),
                pltpu.VMEM((2, heads, HDIM, tokens), jnp.float32),
                pltpu.VMEM((2, heads, 8, tokens), jnp.float32),
                pltpu.SMEM(window.shape, jnp.int32),
                dma((heads, 3)),
                dma,
                dma((max(beside, 1), heads)),
                dma((max(beside, 1), heads)),
                dma((2, heads + 1)),
                dma((2, heads + 1)),
                dma((2, heads)),
                dma((2, heads)),
            ],
            compiler_params=pltpu.CompilerParams(
                collective_id=0, has_side_effects=True, vmem_limit_bytes=VMEM_LIMIT
            ),
        )(*[pltpu.with_memory_space_constraint(a, pltpu.HBM) for a in (queries, keys, values, window)])

    placed = P(("group", "tm"), "space", None, "head")
    return jax.shard_map(
        on_device,
        mesh=mesh,
        in_specs=(placed, placed, placed, P(("group", "tm"), "space", None, None)),
        out_specs=placed,
        check_vma=False,
    )
```

```python
import functools
import math

import jax
import jax.numpy as jnp
from jax import lax
from jax.experimental import pallas as pl
from jax.experimental.pallas import tpu as pltpu
from jax.sharding import PartitionSpec as P

HDIM = 128
TILE = 8
PARTS = 1
EARLY = 1
SHIFT = 0
DIRECT = 0
OWN_LAG, RELAY_LAG, KV_LAG, FAR_LAG, NEAR_LAG = -3, -1, 1, 1, 1
MERGE_LAG, EARLY_LAG, HOME_LAG, LAST_LAG = 2, 1, 1, 5
FORWARD_AT = 0
MASKED = -float(2**17)
EXP2_SCALE = HDIM ** (-0.5) * math.log2(math.e)
VMEM_LIMIT = 40 * 2**20
MESH = pl.DeviceIdType.MESH


def remote(src, dst, send_sem, recv_sem, device):
    return pltpu.make_async_remote_copy(
        src_ref=src,
        dst_ref=dst,
        send_sem=send_sem,
        recv_sem=recv_sem,
        device_id=device,
        device_id_type=MESH,
    )


def kernel(
    frames,
    rows,
    shift,
    q_hbm,
    k_hbm,
    v_hbm,
    win_hbm,
    out_ref,
    q_all,
    kv_all,
    kv_before,
    qb_all,
    kone,
    o_send,
    o_recv,
    lse_send,
    lse_recv,
    o_own,
    lse_own,
    back_send,
    back_recv,
    win_ref,
    ready_sem,
    load_sem,
    win_sem,
    kv_send_sem,
    kv_recv_sem,
    before_send_sem,
    before_recv_sem,
    q_send_sem,
    q_recv_sem,
    qb_send_sem,
    qb_recv_sem,
    o_send_sem,
    o_recv_sem,
    give_send_sem,
    give_recv_sem,
    back_send_sem,
    back_recv_sem,
):
    frame = lax.axis_index("tm")
    row = lax.axis_index("space")
    core = lax.axis_index("head")
    slots = q_all.shape[1]
    heads = slots - shift
    columns = kv_all.shape[4]
    width = columns // PARTS
    span = TILE * width
    tile_cols = columns // TILE
    tokens = TILE * columns
    count = heads + shift * (2 * core - 1) if shift else heads
    has1 = frame + 1 < frames
    has2 = frame + 2 < frames
    prev1 = frame >= 1
    if rows == 1:
        sides = []
    elif rows == 2:
        sides = [(0, 1 - row, None, 1 - 2 * row, 0)]
    else:
        sides = [(0, row - 1, row >= 1, -1, 1), (1, row + 1, row + 1 < rows, 1, 0)]
    blocks = range(1 + len(sides))

    def when(*conditions):
        conditions = [c for c in conditions if c is not None]
        if not conditions:
            return lambda body: body()
        return pl.when(functools.reduce(jnp.logical_and, conditions))

    def lanes_of(head):
        start = head * HDIM
        return pl.ds(start if isinstance(head, int) else pl.multiple_of(start, HDIM), HDIM)

    def pieces(head, slot):
        lanes = lanes_of(head)
        halves = [
            (q_hbm.at[0, :, pl.ds(part * width, width), lanes], q_all.at[0, slot, part])
            for part in range(PARTS)
        ]
        return [
            (k_hbm.at[0, :, :, lanes], kv_all.at[0, slot, 0]),
            (v_hbm.at[0, :, :, lanes], kv_all.at[0, slot, 1]),
        ] + halves

    def load(slot):
        return [
            pltpu.make_async_copy(src, dst, load_sem.at[slot, i])
            for i, (src, dst) in enumerate(pieces(slot, slot))
        ]

    def give(extra):
        return [
            remote(
                src, dst, give_send_sem.at[extra, i], give_recv_sem.at[extra, i], {"head": 1 - core}
            )
            for i, (src, dst) in enumerate(pieces(heads - shift + extra, heads + extra))
        ]

    def give_back(extra):
        return remote(
            back_send.at[extra],
            back_recv.at[extra],
            back_send_sem.at[extra],
            back_recv_sem.at[extra],
            {"head": 1 - core},
        )

    def send_kv(side, slot):
        index, there, _, _, far_index = side
        return remote(
            kv_all.at[0, slot],
            kv_all.at[1 + far_index, slot],
            kv_send_sem.at[index, slot],
            kv_recv_sem.at[far_index, slot],
            {"space": there},
        )

    def got_kv(side, slot):
        index, there, _, _, _ = side
        return remote(
            kv_all.at[0, slot],
            kv_all.at[1 + index, slot],
            kv_send_sem.at[index, slot],
            kv_recv_sem.at[index, slot],
            {"space": there},
        )

    def forward(block, slot):
        return remote(
            kv_all.at[block, slot],
            kv_before.at[block, slot],
            before_send_sem.at[block, slot],
            before_recv_sem.at[block, slot],
            {"tm": frame + 1},
        )

    def send_q(stage, slot, part):
        return remote(
            q_all.at[stage, slot, part],
            q_all.at[stage + 1, slot, part],
            q_send_sem.at[stage, slot, part],
            q_recv_sem.at[stage, slot, part],
            {"tm": frame - 1},
        )

    def send_qb(stage):
        return remote(
            qb_all.at[stage],
            qb_all.at[stage + 1],
            qb_send_sem.at[stage],
            qb_recv_sem.at[stage],
            {"tm": frame - 1},
        )

    def send_o(dt, slot, part, hops=1):
        pairs = ((o_send, o_recv), (lse_send, lse_recv))
        return [
            remote(
                src.at[dt - 1, slot, part],
                dst.at[dt - 1, slot, part],
                o_send_sem.at[dt - 1, slot, part, i],
                o_recv_sem.at[dt - 1, slot, part, i],
                {"tm": frame + hops},
            )
            for i, (src, dst) in enumerate(pairs)
        ]

    def each_slot(body, first=0):
        def step(slot, carry):
            body(slot)
            return carry

        lax.fori_loop(first, count, step, 0)

    partners = [({"space": side[1]}, side[2]) for side in sides]
    if shift:
        partners.append(({"head": 1 - core}, None))
    barrier = pltpu.get_barrier_semaphore()
    for device, there in partners + [({"tm": frame + 1}, has1)]:

        @when(there)
        def _():
            pl.semaphore_signal(barrier, inc=1, device_id=device, device_id_type=MESH)

    window = pltpu.make_async_copy(win_hbm, win_ref, win_sem)
    for slot in range(EARLY + 1):
        for copy in load(slot):
            copy.start()
    window.start()

    def is_local(slot):
        return slot < heads if shift else None

    @functools.partial(each_slot, first=EARLY + 1)
    def _(slot):
        @when(is_local(slot))
        def _():
            for copy in load(slot):
                copy.start()

    peers = sum(
        1 if there is None else jnp.where(there, 1, 0).astype(jnp.int32)
        for there in [there for _, there in partners] + [prev1]
    )
    pl.semaphore_wait(barrier, peers)

    @when(prev1)
    def _():
        pl.semaphore_signal(ready_sem, inc=1, device_id={"tm": frame - 1}, device_id_type=MESH)

    def send_rows(slot):
        for side in sides:

            @when(side[2])
            def _():
                send_kv(side, slot).start()

    def launch(slot):
        for copy in load(slot):
            copy.wait()
        send_rows(slot)

    own_ahead = -OWN_LAG
    first_rest = EARLY + -(-own_ahead // PARTS)

    def send_own(slot):
        @when(prev1)
        def _():
            for part in range(PARTS):
                if (slot - EARLY) * PARTS + part < own_ahead:
                    send_q(0, slot, part).start()

    for slot in range(EARLY + 1):
        launch(slot)
    send_own(EARLY)

    window.wait()
    lane = lax.broadcasted_iota(jnp.int32, (1, HDIM), 1)
    lane_row = lane // tile_cols
    lane_col = lane % tile_cols
    lane_dy = lane_row % 3 - 1
    row_ok = (row + lane_dy >= 0) & (row + lane_dy < rows) & (lane_row < 9)
    col_of = lax.broadcasted_iota(jnp.int32, (columns, 1), 0) // TILE
    table = jnp.zeros((columns, HDIM), jnp.float32)
    for col in range(tile_cols):
        dx = lane_col - col
        near = row_ok & (dx >= -1) & (dx <= 1)
        slot_of_lane = lane_row * 3 + dx + 1
        picked = jnp.zeros((1, HDIM), jnp.int32)
        for slot in range(27):
            picked = jnp.where(slot_of_lane == slot, win_ref[0, 0, col, slot], picked)
        allowed = near & ((picked == 1) | (slot_of_lane == 4))
        offsets = jnp.where(allowed, 0.0, MASKED)
        table = jnp.where(col_of == col, offsets, table)
    for part in range(PARTS):
        qb_all[0, part] = table[part * width : (part + 1) * width].astype(jnp.bfloat16)

    @when(prev1)
    def _():
        send_qb(0).start()

    for slot in range(EARLY + 1, first_rest):
        launch(slot)
        send_own(slot)

    @when(has1)
    def _():
        pl.semaphore_wait(ready_sem, 1)

    @when(has2)
    def _():
        for slot in range(EARLY):
            forward(0, slot).start()

    if shift:

        @when(core == 0)
        def _():
            for extra in range(shift):
                for copy in give(extra):
                    copy.start()

    @functools.partial(each_slot, first=first_rest)
    def _(slot):
        @when(is_local(slot))
        def _():
            for copy in load(slot):
                copy.wait()

        if shift:
            for extra in range(shift):

                @when(slot == heads + extra)
                def _():
                    for copy in give(extra):
                        copy.wait_recv()

        send_rows(slot)

    token = lax.broadcasted_iota(jnp.int32, (tokens, HDIM), 0)
    key_col = (token % columns) // TILE
    key_lane = lax.broadcasted_iota(jnp.int32, (tokens, HDIM), 1)
    for dt in range(3):
        for block, dy in enumerate([0] + [side[3] for side in sides]):
            hot = (dt * 3 + dy + 1) * tile_cols + key_col == key_lane
            kone[dt, pl.ds(block * tokens, tokens), :] = jnp.where(hot, 1.0, 0.0).astype(
                jnp.bfloat16
            )

    for side in sides:
        if side[2] is not None:

            @when(jnp.logical_not(side[2]))
            def _():
                @each_slot
                def _(slot):
                    kv_all[1 + side[0], slot] = jnp.zeros(kv_all.shape[2:], jnp.bfloat16)

                for slot in range(EARLY):
                    kv_before[1 + side[0], slot] = jnp.zeros(kv_before.shape[2:], jnp.bfloat16)

    def attend(stage, dt, slot, part, source):
        query = q_all[stage, slot, part].reshape(span, HDIM)
        offsets = jnp.concatenate([qb_all[stage, part]] * TILE, axis=0)
        query = jnp.concatenate([query, offsets], axis=1)
        key = jnp.concatenate([source[b, slot, 0].reshape(tokens, HDIM) for b in blocks], axis=0)
        key = jnp.concatenate([key, kone[dt]], axis=1)
        value = jnp.concatenate([source[b, slot, 1].reshape(tokens, HDIM) for b in blocks], axis=0)
        scores = lax.dot_general(
            key, query, (((1,), (1,)), ((), ())), preferred_element_type=jnp.float32
        )
        top = jnp.max(scores, axis=0, keepdims=True)
        weights = jnp.exp2((scores - top) * EXP2_SCALE)
        total = jnp.sum(weights, axis=0, keepdims=True)
        part_out = lax.dot_general(
            value,
            weights.astype(jnp.bfloat16),
            (((0,), (0,)), ((), ())),
            preferred_element_type=jnp.float32,
        )
        return part_out / total, top * EXP2_SCALE + jnp.log2(total)

    def pack(dt, slot, part, result, straight=None):
        o_send[dt - 1, slot, part] = result[0].astype(jnp.bfloat16)
        lse_send[dt - 1, slot, part] = result[1]

        @when(None if straight is None else jnp.logical_not(straight))
        def _():
            for copy in send_o(dt, slot, part):
                copy.start()

        if straight is not None:

            @when(straight)
            def _():
                for copy in send_o(dt, slot, part, 2):
                    copy.start()

    def unpack(dt, slot, part):
        for copy in send_o(dt, slot, part):
            copy.wait_recv()
        return o_recv[dt - 1, slot, part].astype(jnp.float32), lse_recv[dt - 1, slot, part]

    def keep(dt, slot, part, result):
        o_own[dt, slot, part] = result[0]
        lse_own[dt, slot, part] = result[1]

    def kept(dt, slot, part):
        return o_own[dt, slot, part], lse_own[dt, slot, part]

    def merge(one, two):
        top = jnp.maximum(one[1], two[1])
        share_one, share_two = jnp.exp2(one[1] - top), jnp.exp2(two[1] - top)
        total = share_one + share_two
        mixed = one[0] * (share_one / total) + two[0] * (share_two / total)
        return mixed, top + jnp.log2(total)

    def finish(slot, part, value):
        done = value.T.astype(jnp.bfloat16).reshape(TILE, width, HDIM)
        here = pl.ds(part * width, width)

        @when(is_local(slot))
        def _():
            out_ref[0, :, here, lanes_of(slot)] = done

        for extra in range(shift):

            @when(slot == heads + extra)
            def _():
                back_send[extra, :, here, :] = done
                if part == PARTS - 1:
                    give_back(extra).start()

    def inside(place):
        return (place >= 0) & (place < count)

    def is_early(place):
        return place >= count - EARLY

    def is_direct(place):
        return (place >= count - EARLY - DIRECT) & (place < count - EARLY)

    def slot_at(place):
        return jnp.where(is_early(place), place - (count - EARLY), place + EARLY)

    def relay(place, part):
        @when(has1, inside(place))
        def _():
            slot = slot_at(place)
            send_q(0, slot, part).wait_recv()

            @when(prev1, jnp.logical_not(is_early(place)))
            def _():
                send_q(1, slot, part).start()

    for n in range(-RELAY_LAG):
        relay(jnp.int32(n // PARTS), n % PARTS)

    @when(has1)
    def _():
        send_qb(0).wait_recv()

        @when(prev1)
        def _():
            send_qb(1).start()

    def step(i, carry):
        for g in range(PARTS):

            def at(lag):
                place = i + (g - lag) // PARTS
                return place, slot_at(place), (g - lag) % PARTS

            @when(i * PARTS + g == FORWARD_AT)
            def _():
                for slot in range(EARLY):
                    for side in sides:

                        @when(side[2])
                        def _():
                            got_kv(side, slot).wait_recv()

                            @when(has2)
                            def _():
                                forward(1 + side[0], slot).start()

            place, slot, part = at(KV_LAG)
            if part == 0:

                @when(inside(place), jnp.logical_not(is_early(place)))
                def _():
                    for side in sides:

                        @when(side[2])
                        def _():
                            got_kv(side, slot).wait_recv()

            place, slot, part = at(FAR_LAG)

            @when(inside(place), has2, jnp.logical_not(is_early(place)))
            def _():
                if part == 0:

                    @when(place == 0)
                    def _():
                        send_qb(1).wait_recv()

                send_q(1, slot, part).wait_recv()
                pack(2, slot, part, attend(2, 2, slot, part, kv_all), is_direct(place))

            relay(*at(RELAY_LAG)[::2])

            place, slot, part = at(NEAR_LAG)

            @when(inside(place), has1)
            def _():
                keep(1, slot, part, attend(1, 1, slot, part, kv_all))

            place, slot, part = at(MERGE_LAG)

            @when(inside(place), has1, jnp.logical_not(is_early(place)))
            def _():
                joins = prev1 & jnp.logical_not(is_direct(place))

                @when(joins)
                def _():
                    pack(1, slot, part, merge(kept(1, slot, part), unpack(2, slot, part)))

                @when(jnp.logical_not(joins))
                def _():
                    pack(1, slot, part, kept(1, slot, part))

            place, slot, part = at(EARLY_LAG)

            @when(inside(place), has1, is_early(place))
            def _():
                @when(prev1)
                def _():
                    if part == 0:
                        got_before(slot)
                    before = attend(1, 2, slot, part, kv_before)
                    pack(1, slot, part, merge(kept(1, slot, part), before))

                @when(jnp.logical_not(prev1))
                def _():
                    pack(1, slot, part, kept(1, slot, part))

            place, slot, part = at(HOME_LAG)

            @when(inside(place))
            def _():
                keep(0, slot, part, attend(0, 0, slot, part, kv_all))

            place, slot, part = at(OWN_LAG)

            @when(prev1, inside(place))
            def _():
                send_q(0, slot, part).start()

            place, slot, part = at(LAST_LAG)

            @when(inside(place))
            def _():
                joins = (frame >= 2) & is_direct(place)

                @when(prev1, jnp.logical_not(joins))
                def _():
                    merged = merge(kept(0, slot, part), unpack(1, slot, part))
                    finish(slot, part, merged[0])

                @when(joins)
                def _():
                    merged = merge(kept(0, slot, part), unpack(1, slot, part))
                    merged = merge(merged, unpack(2, slot, part))
                    finish(slot, part, merged[0])

                @when(jnp.logical_not(prev1))
                def _():
                    finish(slot, part, o_own[0, slot, part])

        return carry

    def got_before(slot):
        forward(0, slot).wait_recv()
        for side in sides:

            @when(side[2])
            def _():
                forward(1 + side[0], slot).wait_recv()

    lax.fori_loop(0, count + -(-LAST_LAG // PARTS), step, 0)

    if shift:

        @when(core == 0)
        def _():
            for extra in range(shift):
                give_back(extra).wait_recv()
                out_ref[0, :, :, lanes_of(heads - shift + extra)] = back_recv[extra]
                for copy in give(extra):
                    copy.wait_send()

        @when(core == 1)
        def _():
            for extra in range(shift):
                give_back(extra).wait_send()

    @when(prev1)
    def _():
        send_qb(0).wait_send()

        @when(has1)
        def _():
            send_qb(1).wait_send()

    @when(has2)
    def _():
        for slot in range(EARLY):
            forward(0, slot).wait_send()
            for side in sides:

                @when(side[2])
                def _():
                    forward(1 + side[0], slot).wait_send()

    @each_slot
    def _(slot):
        for side in sides:

            @when(side[2])
            def _():
                send_kv(side, slot).wait_send()

        for part in range(PARTS):

            @when(prev1)
            def _():
                send_q(0, slot, part).wait_send()

            @when(prev1, has1, slot >= EARLY)
            def _():
                send_q(1, slot, part).wait_send()

            @when(has1)
            def _():
                for copy in send_o(1, slot, part):
                    copy.wait_send()

            @when(has2, slot >= EARLY)
            def _():
                for copy in send_o(2, slot, part):
                    copy.wait_send()


def solution(mesh):
    frames, rows = mesh.shape["tm"], mesh.shape["space"]
    shift = SHIFT if mesh.shape["head"] == 2 else 0

    def on_device(queries, keys, values, window):
        _, _, columns, channels = queries.shape
        slots = channels // HDIM + shift
        tokens = TILE * columns
        span = tokens // PARTS
        beside = min(rows - 1, 2)
        block = (TILE, columns, HDIM)
        spare = max(shift, 1)
        dma = pltpu.SemaphoreType.DMA
        operands = [
            pltpu.with_memory_space_constraint(a, pltpu.HBM)
            for a in (queries, keys, values, window)
        ]
        return pl.pallas_call(
            functools.partial(kernel, frames, rows, shift),
            out_shape=jax.ShapeDtypeStruct(queries.shape, jnp.bfloat16),
            in_specs=[pl.BlockSpec(memory_space=pl.ANY)] * 4,
            out_specs=pl.BlockSpec(memory_space=pltpu.VMEM),
            scratch_shapes=[
                pltpu.VMEM((3, slots, PARTS, TILE, columns // PARTS, HDIM), jnp.bfloat16),
                pltpu.VMEM((1 + beside, slots, 2, *block), jnp.bfloat16),
                pltpu.VMEM((1 + beside, max(EARLY, 1), 2, *block), jnp.bfloat16),
                pltpu.VMEM((3, PARTS, columns // PARTS, HDIM), jnp.bfloat16),
                pltpu.VMEM((3, (1 + beside) * tokens, HDIM), jnp.bfloat16),
                pltpu.VMEM((2, slots, PARTS, HDIM, span), jnp.bfloat16),
                pltpu.VMEM((2, slots, PARTS, HDIM, span), jnp.bfloat16),
                pltpu.VMEM((2, slots, PARTS, 1, span), jnp.float32),
                pltpu.VMEM((2, slots, PARTS, 1, span), jnp.float32),
                pltpu.VMEM((2, slots, PARTS, HDIM, span), jnp.float32),
                pltpu.VMEM((2, slots, PARTS, 1, span), jnp.float32),
                pltpu.VMEM((spare, *block), jnp.bfloat16),
                pltpu.VMEM((spare, *block), jnp.bfloat16),
                pltpu.SMEM(window.shape, jnp.int32),
                pltpu.SemaphoreType.REGULAR,
                dma((slots, 2 + PARTS)),
                dma,
                dma((max(beside, 1), slots)),
                dma((max(beside, 1), slots)),
                dma((1 + beside, max(EARLY, 1))),
                dma((1 + beside, max(EARLY, 1))),
                dma((2, slots, PARTS)),
                dma((2, slots, PARTS)),
                dma((2,)),
                dma((2,)),
                dma((2, slots, PARTS, 2)),
                dma((2, slots, PARTS, 2)),
                dma((spare, 2 + PARTS)),
                dma((spare, 2 + PARTS)),
                dma((spare,)),
                dma((spare,)),
            ],
            compiler_params=pltpu.CompilerParams(
                collective_id=0, has_side_effects=True, vmem_limit_bytes=VMEM_LIMIT
            ),
        )(*operands)

    placed = P(("group", "tm"), "space", None, "head")
    return jax.shard_map(
        on_device,
        mesh=mesh,
        in_specs=(placed, placed, placed, P(("group", "tm"), "space", None, None)),
        out_specs=placed,
        check_vma=False,
    )
```

```python
import functools
import math

import jax
import jax.numpy as jnp
from jax import lax
from jax.experimental import pallas as pl
from jax.experimental.pallas import tpu as pltpu
from jax.sharding import PartitionSpec as P

HDIM = 128
TILE = 8
PARTS = 1
EARLY = 1
SHIFT = 0
DIRECT = 0
OWN_LAG, RELAY_LAG, KV_LAG, FAR_LAG, NEAR_LAG = -3, -1, 1, 1, 1
MERGE_LAG, EARLY_LAG, HOME_LAG, LAST_LAG = 2, 1, 1, 4
FORWARD_AT = 0
MASKED = -float(2**17)
EXP2_SCALE = HDIM ** (-0.5) * math.log2(math.e)
VMEM_LIMIT = 40 * 2**20
MESH = pl.DeviceIdType.MESH


def remote(src, dst, send_sem, recv_sem, device):
    return pltpu.make_async_remote_copy(
        src_ref=src,
        dst_ref=dst,
        send_sem=send_sem,
        recv_sem=recv_sem,
        device_id=device,
        device_id_type=MESH,
    )


def kernel(
    frames,
    rows,
    shift,
    q_hbm,
    k_hbm,
    v_hbm,
    win_hbm,
    out_ref,
    q_all,
    kv_all,
    kv_before,
    qb_all,
    kone,
    o_send,
    o_recv,
    lse_send,
    lse_recv,
    o_own,
    lse_own,
    back_send,
    back_recv,
    win_ref,
    ready_sem,
    load_sem,
    win_sem,
    kv_send_sem,
    kv_recv_sem,
    before_send_sem,
    before_recv_sem,
    q_send_sem,
    q_recv_sem,
    qb_send_sem,
    qb_recv_sem,
    o_send_sem,
    o_recv_sem,
    give_send_sem,
    give_recv_sem,
    back_send_sem,
    back_recv_sem,
):
    frame = lax.axis_index("tm")
    row = lax.axis_index("space")
    core = lax.axis_index("head")
    slots = q_all.shape[1]
    heads = slots - shift
    columns = kv_all.shape[4]
    width = columns // PARTS
    span = TILE * width
    tile_cols = columns // TILE
    tokens = TILE * columns
    count = heads + shift * (2 * core - 1) if shift else heads
    has1 = frame + 1 < frames
    has2 = frame + 2 < frames
    prev1 = frame >= 1
    if rows == 1:
        sides = []
    elif rows == 2:
        sides = [(0, 1 - row, None, 1 - 2 * row, 0)]
    else:
        sides = [(0, row - 1, row >= 1, -1, 1), (1, row + 1, row + 1 < rows, 1, 0)]
    blocks = range(1 + len(sides))

    def when(*conditions):
        conditions = [c for c in conditions if c is not None]
        if not conditions:
            return lambda body: body()
        return pl.when(functools.reduce(jnp.logical_and, conditions))

    def lanes_of(head):
        start = head * HDIM
        return pl.ds(start if isinstance(head, int) else pl.multiple_of(start, HDIM), HDIM)

    def pieces(head, slot):
        lanes = lanes_of(head)
        halves = [
            (q_hbm.at[0, :, pl.ds(part * width, width), lanes], q_all.at[0, slot, part])
            for part in range(PARTS)
        ]
        return [
            (k_hbm.at[0, :, :, lanes], kv_all.at[0, slot, 0]),
            (v_hbm.at[0, :, :, lanes], kv_all.at[0, slot, 1]),
        ] + halves

    def load(slot):
        return [
            pltpu.make_async_copy(src, dst, load_sem.at[slot, i])
            for i, (src, dst) in enumerate(pieces(slot, slot))
        ]

    def give(extra):
        return [
            remote(
                src, dst, give_send_sem.at[extra, i], give_recv_sem.at[extra, i], {"head": 1 - core}
            )
            for i, (src, dst) in enumerate(pieces(heads - shift + extra, heads + extra))
        ]

    def give_back(extra):
        return remote(
            back_send.at[extra],
            back_recv.at[extra],
            back_send_sem.at[extra],
            back_recv_sem.at[extra],
            {"head": 1 - core},
        )

    def send_kv(side, slot):
        index, there, _, _, far_index = side
        return remote(
            kv_all.at[0, slot],
            kv_all.at[1 + far_index, slot],
            kv_send_sem.at[index, slot],
            kv_recv_sem.at[far_index, slot],
            {"space": there},
        )

    def got_kv(side, slot):
        index, there, _, _, _ = side
        return remote(
            kv_all.at[0, slot],
            kv_all.at[1 + index, slot],
            kv_send_sem.at[index, slot],
            kv_recv_sem.at[index, slot],
            {"space": there},
        )

    def forward(block, slot):
        return remote(
            kv_all.at[block, slot],
            kv_before.at[block, slot],
            before_send_sem.at[block, slot],
            before_recv_sem.at[block, slot],
            {"tm": frame + 1},
        )

    def send_q(stage, slot, part):
        return remote(
            q_all.at[stage, slot, part],
            q_all.at[stage + 1, slot, part],
            q_send_sem.at[stage, slot, part],
            q_recv_sem.at[stage, slot, part],
            {"tm": frame - 1},
        )

    def send_qb(stage):
        return remote(
            qb_all.at[stage],
            qb_all.at[stage + 1],
            qb_send_sem.at[stage],
            qb_recv_sem.at[stage],
            {"tm": frame - 1},
        )

    def send_o(dt, slot, part, hops=1):
        pairs = ((lse_send, lse_recv), (o_send, o_recv))
        return [
            remote(
                src.at[dt - 1, slot, part],
                dst.at[dt - 1, slot, part],
                o_send_sem.at[dt - 1, slot, part, i],
                o_recv_sem.at[dt - 1, slot, part, i],
                {"tm": frame + hops},
            )
            for i, (src, dst) in enumerate(pairs)
        ]

    def each_slot(body, first=0):
        def step(slot, carry):
            body(slot)
            return carry

        lax.fori_loop(first, count, step, 0)

    partners = [({"space": side[1]}, side[2]) for side in sides]
    if shift:
        partners.append(({"head": 1 - core}, None))
    barrier = pltpu.get_barrier_semaphore()
    for device, there in partners + [({"tm": frame + 1}, has1)]:

        @when(there)
        def _():
            pl.semaphore_signal(barrier, inc=1, device_id=device, device_id_type=MESH)

    window = pltpu.make_async_copy(win_hbm, win_ref, win_sem)
    for slot in range(EARLY + 1):
        for copy in load(slot):
            copy.start()
    window.start()

    def is_local(slot):
        return slot < heads if shift else None

    @functools.partial(each_slot, first=EARLY + 1)
    def _(slot):
        @when(is_local(slot))
        def _():
            for copy in load(slot):
                copy.start()

    peers = sum(
        1 if there is None else jnp.where(there, 1, 0).astype(jnp.int32)
        for there in [there for _, there in partners] + [prev1]
    )
    pl.semaphore_wait(barrier, peers)

    @when(prev1)
    def _():
        pl.semaphore_signal(ready_sem, inc=1, device_id={"tm": frame - 1}, device_id_type=MESH)

    def send_rows(slot):
        for side in sides:

            @when(side[2])
            def _():
                send_kv(side, slot).start()

    def launch(slot):
        for copy in load(slot):
            copy.wait()
        send_rows(slot)

    own_ahead = -OWN_LAG
    first_rest = EARLY + -(-own_ahead // PARTS)

    def send_own(slot):
        @when(prev1)
        def _():
            for part in range(PARTS):
                if (slot - EARLY) * PARTS + part < own_ahead:
                    send_q(0, slot, part).start()

    for slot in range(EARLY + 1):
        launch(slot)
    send_own(EARLY)

    window.wait()
    lane = lax.broadcasted_iota(jnp.int32, (1, HDIM), 1)
    lane_row = lane // tile_cols
    lane_col = lane % tile_cols
    lane_dy = lane_row % 3 - 1
    row_ok = (row + lane_dy >= 0) & (row + lane_dy < rows) & (lane_row < 9)
    col_of = lax.broadcasted_iota(jnp.int32, (columns, 1), 0) // TILE
    table = jnp.zeros((columns, HDIM), jnp.float32)
    for col in range(tile_cols):
        dx = lane_col - col
        near = row_ok & (dx >= -1) & (dx <= 1)
        slot_of_lane = lane_row * 3 + dx + 1
        picked = jnp.zeros((1, HDIM), jnp.int32)
        for slot in range(27):
            picked = jnp.where(slot_of_lane == slot, win_ref[0, 0, col, slot], picked)
        allowed = near & ((picked == 1) | (slot_of_lane == 4))
        offsets = jnp.where(allowed, 0.0, MASKED)
        table = jnp.where(col_of == col, offsets, table)
    for part in range(PARTS):
        qb_all[0, part] = table[part * width : (part + 1) * width].astype(jnp.bfloat16)

    @when(prev1)
    def _():
        send_qb(0).start()

    for slot in range(EARLY + 1, first_rest):
        launch(slot)
        send_own(slot)

    @when(has1)
    def _():
        pl.semaphore_wait(ready_sem, 1)

    @when(has2)
    def _():
        for slot in range(EARLY):
            forward(0, slot).start()

    if shift:

        @when(core == 0)
        def _():
            for extra in range(shift):
                for copy in give(extra):
                    copy.start()

    @functools.partial(each_slot, first=first_rest)
    def _(slot):
        @when(is_local(slot))
        def _():
            for copy in load(slot):
                copy.wait()

        if shift:
            for extra in range(shift):

                @when(slot == heads + extra)
                def _():
                    for copy in give(extra):
                        copy.wait_recv()

        send_rows(slot)

    token = lax.broadcasted_iota(jnp.int32, (tokens, HDIM), 0)
    key_col = (token % columns) // TILE
    key_lane = lax.broadcasted_iota(jnp.int32, (tokens, HDIM), 1)
    for dt in range(3):
        for block, dy in enumerate([0] + [side[3] for side in sides]):
            hot = (dt * 3 + dy + 1) * tile_cols + key_col == key_lane
            kone[dt, pl.ds(block * tokens, tokens), :] = jnp.where(hot, 1.0, 0.0).astype(
                jnp.bfloat16
            )

    for side in sides:
        if side[2] is not None:

            @when(jnp.logical_not(side[2]))
            def _():
                @each_slot
                def _(slot):
                    kv_all[1 + side[0], slot] = jnp.zeros(kv_all.shape[2:], jnp.bfloat16)

                for slot in range(EARLY):
                    kv_before[1 + side[0], slot] = jnp.zeros(kv_before.shape[2:], jnp.bfloat16)

    def attend(stage, dt, slot, part, source):
        query = q_all[stage, slot, part].reshape(span, HDIM)
        offsets = jnp.concatenate([qb_all[stage, part]] * TILE, axis=0)
        query = jnp.concatenate([query, offsets], axis=1)
        key = jnp.concatenate([source[b, slot, 0].reshape(tokens, HDIM) for b in blocks], axis=0)
        key = jnp.concatenate([key, kone[dt]], axis=1)
        value = jnp.concatenate([source[b, slot, 1].reshape(tokens, HDIM) for b in blocks], axis=0)
        scores = lax.dot_general(
            key, query, (((1,), (1,)), ((), ())), preferred_element_type=jnp.float32
        )
        top = jnp.max(scores, axis=0, keepdims=True)
        weights = jnp.exp2((scores - top) * EXP2_SCALE)
        total = jnp.sum(weights, axis=0, keepdims=True)
        part_out = lax.dot_general(
            value,
            weights.astype(jnp.bfloat16),
            (((0,), (0,)), ((), ())),
            preferred_element_type=jnp.float32,
        )
        return part_out / total, top * EXP2_SCALE + jnp.log2(total)

    def pack(dt, slot, part, result, straight=None):
        o_send[dt - 1, slot, part] = result[0].astype(jnp.bfloat16)
        lse_send[dt - 1, slot, part] = result[1]

        @when(None if straight is None else jnp.logical_not(straight))
        def _():
            for copy in send_o(dt, slot, part):
                copy.start()

        if straight is not None:

            @when(straight)
            def _():
                for copy in send_o(dt, slot, part, 2):
                    copy.start()

    def unpack(dt, slot, part):
        for copy in send_o(dt, slot, part):
            copy.wait_recv()
        return o_recv[dt - 1, slot, part].astype(jnp.float32), lse_recv[dt - 1, slot, part]

    def keep(dt, slot, part, result):
        o_own[dt, slot, part] = result[0]
        lse_own[dt, slot, part] = result[1]

    def kept(dt, slot, part):
        return o_own[dt, slot, part], lse_own[dt, slot, part]

    def merge(one, two):
        top = jnp.maximum(one[1], two[1])
        share_one, share_two = jnp.exp2(one[1] - top), jnp.exp2(two[1] - top)
        total = share_one + share_two
        mixed = one[0] * (share_one / total) + two[0] * (share_two / total)
        return mixed, top + jnp.log2(total)

    def finish(slot, part, value):
        done = value.T.astype(jnp.bfloat16).reshape(TILE, width, HDIM)
        here = pl.ds(part * width, width)

        @when(is_local(slot))
        def _():
            out_ref[0, :, here, lanes_of(slot)] = done

        for extra in range(shift):

            @when(slot == heads + extra)
            def _():
                back_send[extra, :, here, :] = done
                if part == PARTS - 1:
                    give_back(extra).start()

    def inside(place):
        return (place >= 0) & (place < count)

    def is_early(place):
        return place >= count - EARLY

    def is_direct(place):
        return (place >= count - EARLY - DIRECT) & (place < count - EARLY)

    def slot_at(place):
        return jnp.where(is_early(place), place - (count - EARLY), place + EARLY)

    def relay(place, part):
        @when(has1, inside(place))
        def _():
            slot = slot_at(place)
            send_q(0, slot, part).wait_recv()

            @when(prev1, jnp.logical_not(is_early(place)))
            def _():
                send_q(1, slot, part).start()

    for n in range(-RELAY_LAG):
        relay(jnp.int32(n // PARTS), n % PARTS)

    @when(has1)
    def _():
        send_qb(0).wait_recv()

        @when(prev1)
        def _():
            send_qb(1).start()

    def step(i, carry):
        for g in range(PARTS):

            def at(lag):
                place = i + (g - lag) // PARTS
                return place, slot_at(place), (g - lag) % PARTS

            @when(i * PARTS + g == FORWARD_AT)
            def _():
                for slot in range(EARLY):
                    for side in sides:

                        @when(side[2])
                        def _():
                            got_kv(side, slot).wait_recv()

                            @when(has2)
                            def _():
                                forward(1 + side[0], slot).start()

            place, slot, part = at(KV_LAG)
            if part == 0:

                @when(inside(place), jnp.logical_not(is_early(place)))
                def _():
                    for side in sides:

                        @when(side[2])
                        def _():
                            got_kv(side, slot).wait_recv()

            place, slot, part = at(FAR_LAG)

            @when(inside(place), has2, jnp.logical_not(is_early(place)))
            def _():
                if part == 0:

                    @when(place == 0)
                    def _():
                        send_qb(1).wait_recv()

                send_q(1, slot, part).wait_recv()
                pack(2, slot, part, attend(2, 2, slot, part, kv_all), is_direct(place))

            relay(*at(RELAY_LAG)[::2])

            place, slot, part = at(NEAR_LAG)

            @when(inside(place), has1)
            def _():
                keep(1, slot, part, attend(1, 1, slot, part, kv_all))

            place, slot, part = at(MERGE_LAG)

            @when(inside(place), has1, jnp.logical_not(is_early(place)))
            def _():
                joins = prev1 & jnp.logical_not(is_direct(place))

                @when(joins)
                def _():
                    pack(1, slot, part, merge(kept(1, slot, part), unpack(2, slot, part)))

                @when(jnp.logical_not(joins))
                def _():
                    pack(1, slot, part, kept(1, slot, part))

            place, slot, part = at(EARLY_LAG)

            @when(inside(place), has1, is_early(place))
            def _():
                @when(prev1)
                def _():
                    if part == 0:
                        got_before(slot)
                    before = attend(1, 2, slot, part, kv_before)
                    pack(1, slot, part, merge(kept(1, slot, part), before))

                @when(jnp.logical_not(prev1))
                def _():
                    pack(1, slot, part, kept(1, slot, part))

            place, slot, part = at(HOME_LAG)

            @when(inside(place))
            def _():
                keep(0, slot, part, attend(0, 0, slot, part, kv_all))

            place, slot, part = at(OWN_LAG)

            @when(prev1, inside(place))
            def _():
                send_q(0, slot, part).start()

            place, slot, part = at(LAST_LAG)

            @when(inside(place))
            def _():
                joins = (frame >= 2) & is_direct(place)

                @when(prev1, jnp.logical_not(joins))
                def _():
                    merged = merge(kept(0, slot, part), unpack(1, slot, part))
                    finish(slot, part, merged[0])

                @when(joins)
                def _():
                    merged = merge(kept(0, slot, part), unpack(1, slot, part))
                    merged = merge(merged, unpack(2, slot, part))
                    finish(slot, part, merged[0])

                @when(jnp.logical_not(prev1))
                def _():
                    finish(slot, part, o_own[0, slot, part])

        return carry

    def got_before(slot):
        forward(0, slot).wait_recv()
        for side in sides:

            @when(side[2])
            def _():
                forward(1 + side[0], slot).wait_recv()

    lax.fori_loop(0, count + -(-LAST_LAG // PARTS), step, 0)

    if shift:

        @when(core == 0)
        def _():
            for extra in range(shift):
                give_back(extra).wait_recv()
                out_ref[0, :, :, lanes_of(heads - shift + extra)] = back_recv[extra]
                for copy in give(extra):
                    copy.wait_send()

        @when(core == 1)
        def _():
            for extra in range(shift):
                give_back(extra).wait_send()

    @when(prev1)
    def _():
        send_qb(0).wait_send()

        @when(has1)
        def _():
            send_qb(1).wait_send()

    @when(has2)
    def _():
        for slot in range(EARLY):
            forward(0, slot).wait_send()
            for side in sides:

                @when(side[2])
                def _():
                    forward(1 + side[0], slot).wait_send()

    @each_slot
    def _(slot):
        for side in sides:

            @when(side[2])
            def _():
                send_kv(side, slot).wait_send()

        for part in range(PARTS):

            @when(prev1)
            def _():
                send_q(0, slot, part).wait_send()

            @when(prev1, has1, slot >= EARLY)
            def _():
                send_q(1, slot, part).wait_send()

            @when(has1)
            def _():
                for copy in send_o(1, slot, part):
                    copy.wait_send()

            @when(has2, slot >= EARLY)
            def _():
                for copy in send_o(2, slot, part):
                    copy.wait_send()


def solution(mesh):
    frames, rows = mesh.shape["tm"], mesh.shape["space"]
    shift = SHIFT if mesh.shape["head"] == 2 else 0

    def on_device(queries, keys, values, window):
        _, _, columns, channels = queries.shape
        slots = channels // HDIM + shift
        tokens = TILE * columns
        span = tokens // PARTS
        beside = min(rows - 1, 2)
        block = (TILE, columns, HDIM)
        spare = max(shift, 1)
        dma = pltpu.SemaphoreType.DMA
        operands = [
            pltpu.with_memory_space_constraint(a, pltpu.HBM)
            for a in (queries, keys, values, window)
        ]
        return pl.pallas_call(
            functools.partial(kernel, frames, rows, shift),
            out_shape=jax.ShapeDtypeStruct(queries.shape, jnp.bfloat16),
            in_specs=[pl.BlockSpec(memory_space=pl.ANY)] * 4,
            out_specs=pl.BlockSpec(memory_space=pltpu.VMEM),
            scratch_shapes=[
                pltpu.VMEM((3, slots, PARTS, TILE, columns // PARTS, HDIM), jnp.bfloat16),
                pltpu.VMEM((1 + beside, slots, 2, *block), jnp.bfloat16),
                pltpu.VMEM((1 + beside, max(EARLY, 1), 2, *block), jnp.bfloat16),
                pltpu.VMEM((3, PARTS, columns // PARTS, HDIM), jnp.bfloat16),
                pltpu.VMEM((3, (1 + beside) * tokens, HDIM), jnp.bfloat16),
                pltpu.VMEM((2, slots, PARTS, HDIM, span), jnp.bfloat16),
                pltpu.VMEM((2, slots, PARTS, HDIM, span), jnp.bfloat16),
                pltpu.VMEM((2, slots, PARTS, 1, span), jnp.float32),
                pltpu.VMEM((2, slots, PARTS, 1, span), jnp.float32),
                pltpu.VMEM((2, slots, PARTS, HDIM, span), jnp.float32),
                pltpu.VMEM((2, slots, PARTS, 1, span), jnp.float32),
                pltpu.VMEM((spare, *block), jnp.bfloat16),
                pltpu.VMEM((spare, *block), jnp.bfloat16),
                pltpu.SMEM(window.shape, jnp.int32),
                pltpu.SemaphoreType.REGULAR,
                dma((slots, 2 + PARTS)),
                dma,
                dma((max(beside, 1), slots)),
                dma((max(beside, 1), slots)),
                dma((1 + beside, max(EARLY, 1))),
                dma((1 + beside, max(EARLY, 1))),
                dma((2, slots, PARTS)),
                dma((2, slots, PARTS)),
                dma((2,)),
                dma((2,)),
                dma((2, slots, PARTS, 2)),
                dma((2, slots, PARTS, 2)),
                dma((spare, 2 + PARTS)),
                dma((spare, 2 + PARTS)),
                dma((spare,)),
                dma((spare,)),
            ],
            compiler_params=pltpu.CompilerParams(
                collective_id=0, has_side_effects=True, vmem_limit_bytes=VMEM_LIMIT
            ),
        )(*operands)

    placed = P(("group", "tm"), "space", None, "head")
    return jax.shard_map(
        on_device,
        mesh=mesh,
        in_specs=(placed, placed, placed, P(("group", "tm"), "space", None, None)),
        out_specs=placed,
        check_vma=False,
    )
```
